512 devices in a mesh: grp: 8 (over x, y_hi), blk: 64 (over y_lo, z, core).
Axes of the slice: x: 4, y: 8 (y_hi: 2, y_lo: 4; y = y_hi * 4 + y_lo), z: 8, core: 2. Of those that a mesh axis runs over, the one named last changes fastest.
Arguments:
- params: bfloat16 [8, 7168, 4096], P('grp', 'blk'), may hold values from -0.0625 to 0.0625
- tracker: bfloat16 [8, 7168, 4096], P('grp', 'blk'), may hold values from -0.29882812 to 0.29882812
- hidden: bfloat16 [1024, 7168], P('grp', 'blk'), may hold values from -6 to 6
- target: bfloat16 [1024, 4096], P('grp'), may hold values from -6 to 6
Outputs:
- params_next: bfloat16 [8, 7168, 4096], P('grp', 'blk')
- tracker_next: bfloat16 [8, 7168, 4096], P('grp', 'blk')
The draws below stay inside these ranges and needn't reach their ends.
All inputs are finite; a program needn't handle non-finite values.
Results may differ from the reference program's by a relative error of at most 0.01.
Values may be sent and summed in bfloat16 or wider, within the bound.
A program may use at most 128 MiB of HBM per device.

```python
import jax
import jax.numpy as jnp
from jax import lax

D = 4096
FF_WIN = 7168
TOK = 128
ALL_TOK = 1024
N_GRP = 8


def levels(rng, extent, split, smallest, largest):
    def one(position, parts):
        draws = jax.random.uniform(jax.random.fold_in(jax.random.fold_in(rng, 6), position), (parts,), jnp.float32, smallest / len(split), largest / len(split))
        return jnp.repeat(jnp.exp(draws), extent[position] // parts).reshape((-1,) + (1,) * (len(extent) - position - 1))

    loudness = one(*split[0])
    for cut in split[1:]:
        loudness = loudness * one(*cut)
    return loudness


def noise(key, shape, width, bound, split=(), dtype=jnp.bfloat16):
    gain = levels(key, shape, split, -0.22, 0.18) if split else 1.0
    entries = jax.random.normal(key, shape, jnp.float32) * width * gain
    return jnp.minimum(jnp.maximum(entries, -bound), bound).astype(dtype)


def setup_inputs(seed: int = 0) -> dict:
    key_of = jax.random.split(jax.random.key(seed), 5)
    return {
        "params": noise(key_of[0], (N_GRP, FF_WIN, D), FF_WIN ** -0.5, 0.0625, ((0, 8), (1, 64))),
        "tracker": noise(key_of[1], (N_GRP, FF_WIN, D), 0.05, 0.29882812, ((0, 8), (1, 64))),
        "hidden": noise(key_of[2], (ALL_TOK, FF_WIN), 1.0, 6.0, ((0, 8), (1, 64))),
        "target": noise(key_of[3], (ALL_TOK, D), 1.0, 6.0, ((0, 8),)),
    }


step_size = 0.05


def mix(value):
    count = value.shape[0]
    zero_row = jnp.zeros_like(value[:1])
    left = jnp.concatenate([zero_row, value[:-1]], 0)
    right = jnp.concatenate([value[1:], zero_row], 0)
    place = jnp.arange(count)
    has_left = (place > 0).astype(jnp.float32)[:, None, None]
    has_right = (place < count - 1).astype(jnp.float32)[:, None, None]
    return value + has_left * (left - value) / 3.0 + has_right * (right - value) / 3.0


def gradient(weights, hidden_rows, target_rows):
    output = jnp.dot(hidden_rows, weights, preferred_element_type=jnp.float32)
    resid = jnp.tanh(output - target_rows.astype(jnp.float32)).astype(jnp.bfloat16)
    total = lax.dot_general(hidden_rows, resid, (((0,), (0,)), ((), ())), preferred_element_type=jnp.float32)
    return total / TOK


def reference(params, tracker, hidden, target):
    groups = params.shape[0]
    olds = []
    for replica in range(groups):
        olds.append(gradient(params[replica], hidden[replica * TOK:(replica + 1) * TOK], target[replica * TOK:(replica + 1) * TOK]))
    params_next = (mix(mix(params.astype(jnp.float32))) - step_size * tracker.astype(jnp.float32)).astype(jnp.bfloat16)
    mixed_tracker = mix(mix(tracker.astype(jnp.float32)))
    outcome = []
    for replica in range(groups):
        fresh = gradient(params_next[replica], hidden[replica * TOK:(replica + 1) * TOK], target[replica * TOK:(replica + 1) * TOK])
        outcome.append(mixed_tracker[replica] + fresh - olds[replica])
    tracker_next = jnp.stack(outcome).astype(jnp.bfloat16)
    return params_next, tracker_next
```

```python
import jax
import jax.numpy as jnp
from jax import lax
from jax.experimental import pallas as pl
from jax.experimental.pallas import tpu as pltpu
from jax.sharding import PartitionSpec as P

step_size = 0.05
MESH = pl.DeviceIdType.MESH
F32 = jnp.float32
BF16 = jnp.bfloat16

RUN = 4
RING = 8
CORES = 2
CHUNK = 1024
HALF = CHUNK // CORES
PIECE = HALF // RUN


def step_kernel(
    params, tracker, hidden, target,
    params_next, tracker_next,
    p_own, t_own, h_own, tgt, h_turned,
    p_across, p_side, u_out, u_in, p_new,
    t_side, w_out, w_in, t_new,
    grad,
    core_out, core_keep, core_in, z_out, z_in, y_out, y_in, resid_old,
    gather_own, gather_other,
    in_sem, out_sem,
    pair_s, pair_r, row_s, row_r, u_s, u_r, tx_s, tx_r, ty_s, ty_r,
    core_s, core_r, z_s, z_r, y_s, y_r, gy_s, gy_r, gz_s, gz_r, gc_s, gc_r,
):
    rows, width = p_own.shape
    tokens = h_own.shape[0]
    strip = tokens // RING
    steps = width // CHUNK
    blocks = width // HALF
    group, place = lax.axis_index("grp"), lax.axis_index("blk")
    n_grp = lax.axis_size("grp")
    columns = n_grp // 2
    x, side = group // 2, lax.rem(group, 2)
    run, rest = place // (RING * CORES), lax.rem(place, RING * CORES)
    ring, core = rest // CORES, lax.rem(rest, CORES)
    s = 1 - 2 * side

    def at_blk(run_, ring_, core_):
        return (group, (run_ * RING + ring_) * CORES + core_)

    partner = at_blk(run, ring, 1 - core)
    ring_peer = [at_blk(run, lax.rem(ring + j, RING), core) for j in range(1, RING)]
    ring_at = [lax.rem(ring + j, RING) for j in range(1, RING)]
    run_peer = [at_blk(lax.rem(run + j, RUN), ring, core) for j in range(1, RUN)]
    run_at = [lax.rem(run + j, RUN) for j in range(1, RUN)]
    across = (x * 2 + (1 - side), place)
    ahead = (lax.rem(x + s + columns, columns) * 2 + side, place)
    behind = (lax.rem(x - s + columns, columns) * 2 + side, place)

    barrier = pltpu.get_barrier_semaphore()
    peers = [across, ahead, behind, partner] + run_peer + ring_peer
    for peer in peers:
        pl.semaphore_signal(barrier, inc=1, device_id=peer, device_id_type=MESH)

    def piece_column(k):
        return pl.multiple_of(k * CHUNK + core * HALF + run * PIECE, PIECE)

    ring_rows = pl.ds(pl.multiple_of(ring * strip, strip), strip)
    loads = [
        pltpu.make_async_copy(params, p_own, in_sem.at[0]),
        pltpu.make_async_copy(tracker, t_own, in_sem.at[1]),
        pltpu.make_async_copy(hidden, h_own, in_sem.at[2]),
    ] + [
        pltpu.make_async_copy(
            target.at[ring_rows, pl.ds(piece_column(k), PIECE)], tgt.at[k], in_sem.at[3 + k]
        )
        for k in range(steps)
    ]
    for load in loads:
        load.start()

    def remote(src, dst, send, recv, peer):
        return pltpu.make_async_remote_copy(
            src_ref=src, dst_ref=dst, send_sem=send, recv_sem=recv, device_id=peer, device_id_type=MESH
        )

    def cols(k, w):
        return pl.ds(k * w, w)

    def valid(i):
        return jnp.where((i >= 0) & (i < n_grp), 1.0, 0.0).astype(F32)

    def keep(i):
        return 1.0 - (valid(i - 1) + valid(i + 1)) / 3.0

    third = 1.0 / 3.0
    c_own = keep(group) * keep(group) + (valid(group - 1) + valid(group + 1)) / 9.0
    c_pair = (keep(group) + keep(group + s)) * third
    c_ahead = valid(group + 2 * s) / 9.0
    c_behind = valid(group - 2 * s) / 9.0
    c_next = (keep(group + s) + keep(group + 2 * s)) * third * valid(group + 2 * s)

    sent = []

    def go(copy):
        copy.start()
        sent.append(copy)
        return copy

    pair, row, u, tx, ty = {}, {}, {}, {}, {}
    core_copy, z_copy, y_copy, gy, gz, gc = {}, {}, {}, {}, {}, {}
    outs = []

    def send_tx(k, d):
        c = cols(k, CHUNK)
        tx[k, d] = go(remote(
            t_own.at[:, c], t_side.at[d, :, c], tx_s.at[d, k], tx_r.at[d, k], behind if d == 0 else ahead
        ))

    def outputs(p, k):
        weights = p_own if p == 0 else p_new
        for half in range(CORES):
            c = cols(k * CORES + half, HALF)
            part = jnp.dot(h_own[...], weights[:, c], preferred_element_type=F32)
            core_keep[p, k, half] = part
            core_out[p, k, half] = part.astype(BF16)
        core_copy[p, k] = go(remote(
            core_out.at[p, k, 1 - core], core_in.at[p, k], core_s.at[p, k], core_r.at[p, k], partner
        ))

    def across_ring(p, k):
        core_copy[p, k].wait_recv()
        z_out[p, k] = (core_keep[p, k, core] + core_in[p, k].astype(F32)).astype(BF16)
        for j in range(RING - 1):
            part = pl.ds(pl.multiple_of(ring_at[j] * strip, strip), strip)
            z_copy[p, k, j] = go(remote(
                z_out.at[p, k, part], z_in.at[p, k, j], z_s.at[p, k, j], z_r.at[p, k, j], ring_peer[j]
            ))

    def across_run(p, k):
        total = z_out[p, k, ring_rows].astype(F32)
        for j in range(RING - 1):
            z_copy[p, k, j].wait_recv()
            total += z_in[p, k, j].astype(F32)
        y_out[p, k] = total.astype(BF16)
        for j in range(RUN - 1):
            part = pl.ds(pl.multiple_of(run_at[j] * PIECE, PIECE), PIECE)
            y_copy[p, k, j] = go(remote(
                y_out.at[p, k, :, part], y_in.at[p, k, j], y_s.at[p, k, j], y_r.at[p, k, j], run_peer[j]
            ))

    own_piece = pl.ds(pl.multiple_of(run * PIECE, PIECE), PIECE)

    def residual(p, k):
        total = y_out[p, k, :, own_piece].astype(F32)
        for j in range(RUN - 1):
            y_copy[p, k, j].wait_recv()
            total += y_in[p, k, j].astype(F32)
        resid = jnp.tanh(total - tgt[k].astype(F32))
        if p == 0:
            resid_old[k] = resid
            return
        gather_own[k, ring_rows, own_piece] = (resid - resid_old[k]).astype(BF16)
        block = gather_own.at[k, ring_rows, own_piece]
        for j in range(RUN - 1):
            gy[k, j] = go(remote(block, block, gy_s.at[k, j], gy_r.at[k, j], run_peer[j]))

    def back_ring(k):
        for j in range(RUN - 1):
            gy[k, j].wait_recv()
        block = gather_own.at[k, ring_rows]
        for j in range(RING - 1):
            gz[k, j] = go(remote(block, block, gz_s.at[k, j], gz_r.at[k, j], ring_peer[j]))

    def back_core(k):
        for j in range(RING - 1):
            gz[k, j].wait_recv()
        gc[k] = go(remote(gather_own.at[k], gather_other.at[k], gc_s.at[k], gc_r.at[k], partner))
        c = pl.ds(pl.multiple_of(k * CHUNK + core * HALF, HALF), HALF)
        grad[:, c] = jnp.dot(h_turned[...], gather_own[k], preferred_element_type=F32)

    def last_grad(k):
        gc[k].wait_recv()
        c = pl.ds(pl.multiple_of(k * CHUNK + (1 - core) * HALF, HALF), HALF)
        grad[:, c] = jnp.dot(h_turned[...], gather_other[k], preferred_element_type=F32)

    def send_u(k):
        c = cols(k, CHUNK)
        pair[k].wait_recv()
        u_out[:, c] = (c_ahead * p_own[:, c].astype(F32) + c_next * p_across[:, c].astype(F32)).astype(BF16)
        u[k] = go(remote(u_out.at[:, c], u_in.at[:, c], u_s.at[k], u_r.at[k], ahead))

    def new_params(k):
        c = cols(k, CHUNK)
        row[k].wait_recv()
        u[k].wait_recv()
        mixed = c_own * p_own[:, c].astype(F32) + c_pair * p_across[:, c].astype(F32)
        mixed += c_ahead * p_side[:, c].astype(F32) + u_in[:, c].astype(F32)
        p_new[:, c] = (mixed - step_size * t_own[:, c].astype(F32)).astype(BF16)
        store = pltpu.make_async_copy(p_new.at[:, c], params_next.at[:, c], out_sem.at[0, k])
        store.start()
        outs.append(store)

    seen = set()

    def send_ty(b):
        k = b * HALF // CHUNK
        if k not in seen:
            tx[k, 0].wait_recv()
            seen.add(k)
        c = cols(b, HALF)
        w_out[:, c] = (c_pair * t_own[:, c].astype(F32) + c_next * t_side[0, :, c].astype(F32)).astype(BF16)
        ty[b] = go(remote(w_out.at[:, c], w_in.at[:, c], ty_s.at[b], ty_r.at[b], across))

    def new_tracker(b):
        c = cols(b, HALF)
        ty[b].wait_recv()
        mixed = c_own * t_own[:, c].astype(F32) + c_ahead * t_side[0, :, c].astype(F32)
        mixed += c_behind * t_side[1, :, c].astype(F32) + w_in[:, c].astype(F32)
        t_new[:, c] = (mixed + grad[:, c] * (1.0 / tokens)).astype(BF16)
        store = pltpu.make_async_copy(t_new.at[:, c], tracker_next.at[:, c], out_sem.at[1, b])
        store.start()
        outs.append(store)

    loads[0].wait()
    pl.semaphore_wait(barrier, len(peers))
    for k in range(steps):
        c = cols(k, CHUNK)
        pair[k] = go(remote(p_own.at[:, c], p_across.at[:, c], pair_s.at[k], pair_r.at[k], across))
    for k in range(steps):
        c = cols(k, CHUNK)
        row[k] = go(remote(p_own.at[:, c], p_side.at[:, c], row_s.at[k], row_r.at[k], behind))
    loads[1].wait()
    for k in range(steps):
        send_tx(k, 0)
    for k in range(2):
        send_tx(k, 1)
    loads[2].wait()
    h_turned[...] = h_own[...].astype(F32).T.astype(BF16)
    for load in loads[3:]:
        load.wait()
    for k in range(steps):
        outputs(0, k)
    for k in range(steps):
        across_ring(0, k)
    send_u(0)
    send_tx(2, 1)
    for k in range(steps):
        across_run(0, k)
    new_params(0)
    outputs(1, 0)
    across_ring(1, 0)
    send_u(1)
    send_tx(3, 1)
    new_params(1)
    outputs(1, 1)
    across_ring(1, 1)
    across_run(1, 0)
    send_u(2)
    new_params(2)
    outputs(1, 2)
    across_ring(1, 2)
    across_run(1, 1)
    send_ty(0)
    send_ty(1)
    send_u(3)
    new_params(3)
    outputs(1, 3)
    across_ring(1, 3)
    for k in range(steps):
        residual(0, k)
    residual(1, 0)
    residual(1, 1)
    across_run(1, 2)
    send_ty(2)
    back_ring(0)
    back_ring(1)
    across_run(1, 3)
    send_ty(3)
    residual(1, 2)
    residual(1, 3)
    send_ty(4)
    send_ty(5)
    send_ty(6)
    send_ty(7)
    back_ring(2)
    back_core(0)
    back_core(1)
    last_grad(0)
    last_grad(1)
    back_ring(3)
    back_core(2)
    last_grad(2)
    for k in range(steps):
        tx[k, 1].wait_recv()
    for b in range(4):
        new_tracker(b)
    back_core(3)
    last_grad(3)
    for b in range(4, blocks):
        new_tracker(b)
    for copy in sent:
        copy.wait_send()
    for store in outs:
        store.wait()


def body(params, tracker, hidden, target):
    _, rows, width = params.shape
    tokens = hidden.shape[0]
    steps, blocks = width // CHUNK, width // HALF
    strip = tokens // RING
    any_ = pl.BlockSpec(memory_space=pl.ANY)
    dma = pltpu.SemaphoreType.DMA
    whole = pltpu.VMEM((rows, width), BF16)
    scratch = [
        whole, whole, pltpu.VMEM(hidden.shape, BF16), pltpu.VMEM((steps, strip, PIECE), BF16),
        pltpu.VMEM((rows, tokens), BF16),
        whole, whole, whole, whole, whole,
        pltpu.VMEM((2, rows, width), BF16), whole, whole, whole,
        pltpu.VMEM((rows, width), F32),
        pltpu.VMEM((2, steps, CORES, tokens, HALF), BF16), pltpu.VMEM((2, steps, CORES, tokens, HALF), F32),
        pltpu.VMEM((2, steps, tokens, HALF), BF16), pltpu.VMEM((2, steps, tokens, HALF), BF16),
        pltpu.VMEM((2, steps, RING - 1, strip, HALF), BF16),
        pltpu.VMEM((2, steps, strip, HALF), BF16), pltpu.VMEM((2, steps, RUN - 1, strip, PIECE), BF16),
        pltpu.VMEM((steps, strip, PIECE), F32),
        pltpu.VMEM((steps, tokens, HALF), BF16), pltpu.VMEM((steps, tokens, HALF), BF16),
        dma((3 + steps,)), dma((2, blocks)),
    ]
    for shape in (
        (steps,), (steps,), (steps,), (2, steps), (blocks,),
        (2, steps), (2, steps, RING - 1), (2, steps, RUN - 1),
        (steps, RUN - 1), (steps, RING - 1), (steps,),
    ):
        scratch += [dma(shape), dma(shape)]
    out = jax.ShapeDtypeStruct((rows, width), BF16)
    params_next, tracker_next = pl.pallas_call(
        step_kernel,
        out_shape=(out, out),
        in_specs=[any_] * 4,
        out_specs=(any_, any_),
        scratch_shapes=scratch,
        name="tracking_step",
        compiler_params=pltpu.CompilerParams(collective_id=0, has_side_effects=True, vmem_limit_bytes=60 << 20),
    )(params[0], tracker[0], hidden, target)
    return params_next[None], tracker_next[None]


def solution(mesh):
    placed = (P("grp", "blk", None), P("grp", "blk", None), P("grp", "blk"), P("grp", None))
    return jax.shard_map(
        body,
        mesh=mesh,
        in_specs=placed,
        out_specs=(P("grp", "blk", None), P("grp", "blk", None)),
        check_vma=False,
    )
```

```python
import jax
import jax.numpy as jnp
from jax import lax
from jax.experimental import pallas as pl
from jax.experimental.pallas import tpu as pltpu
from jax.sharding import PartitionSpec as P

step_size = 0.05
MESH = pl.DeviceIdType.MESH
F32 = jnp.float32
BF16 = jnp.bfloat16

RUN = 4
RING = 8
CORES = 2
SCOPES = False
RAW = 2
CHUNK = 1024
HALF = CHUNK // CORES
PIECE = HALF // RUN


def step_kernel(
    params, tracker, hidden, target,
    params_next, tracker_next,
    p_own, t_own, h_own, tgt, h_turned,
    p_across, p_side, u_out, u_in,
    t_side, w_out, w_in,
    grad,
    core_out, core_keep, core_in, z_out, z_in, y_out, y_in, resid_old,
    gather_own, gather_other,
    in_sem,
    pair_s, pair_r, row_s, row_r, u_s, u_r, tx_s, tx_r, ty_s, ty_r,
    core_s, core_r, z_s, z_r, y_s, y_r, gy_s, gy_r, gz_s, gz_r, gc_s, gc_r,
):
    rows, width = p_own.shape
    tokens = h_own.shape[0]
    strip = tokens // RING
    steps = width // CHUNK
    blocks = width // HALF
    group, place = lax.axis_index("grp"), lax.axis_index("blk")
    n_grp = lax.axis_size("grp")
    columns = n_grp // 2
    x, side = group // 2, lax.rem(group, 2)
    run, rest = place // (RING * CORES), lax.rem(place, RING * CORES)
    ring, core = rest // CORES, lax.rem(rest, CORES)
    s = 1 - 2 * side

    def at_blk(run_, ring_, core_):
        return (group, (run_ * RING + ring_) * CORES + core_)

    partner = at_blk(run, ring, 1 - core)
    ring_peer = [at_blk(run, lax.rem(ring + j, RING), core) for j in range(1, RING)]
    ring_at = [lax.rem(ring + j, RING) for j in range(1, RING)]
    run_peer = [at_blk(lax.rem(run + j, RUN), ring, core) for j in range(1, RUN)]
    run_at = [lax.rem(run + j, RUN) for j in range(1, RUN)]
    across = (x * 2 + (1 - side), place)
    ahead = (lax.rem(x + s + columns, columns) * 2 + side, place)
    behind = (lax.rem(x - s + columns, columns) * 2 + side, place)

    barrier = pltpu.get_barrier_semaphore()
    peers = [across, ahead, behind, partner] + run_peer + ring_peer
    for peer in peers:
        pl.semaphore_signal(barrier, inc=1, device_id=peer, device_id_type=MESH)

    def piece_column(k):
        return pl.multiple_of(k * CHUNK + core * HALF + run * PIECE, PIECE)

    ring_rows = pl.ds(pl.multiple_of(ring * strip, strip), strip)
    loads = [
        pltpu.make_async_copy(params, p_own, in_sem.at[0]),
        pltpu.make_async_copy(tracker, t_own, in_sem.at[1]),
        pltpu.make_async_copy(hidden, h_turned, in_sem.at[2]),
    ] + [
        pltpu.make_async_copy(
            target.at[ring_rows, pl.ds(piece_column(k), PIECE)], tgt.at[k], in_sem.at[3 + k]
        )
        for k in range(steps)
    ]
    for load in loads:
        load.start()

    def remote(src, dst, send, recv, peer):
        return pltpu.make_async_remote_copy(
            src_ref=src, dst_ref=dst, send_sem=send, recv_sem=recv, device_id=peer, device_id_type=MESH
        )

    def cols(k, w):
        return pl.ds(k * w, w)

    def valid(i):
        return jnp.where((i >= 0) & (i < n_grp), 1.0, 0.0).astype(F32)

    def keep(i):
        return 1.0 - (valid(i - 1) + valid(i + 1)) / 3.0

    third = 1.0 / 3.0
    c_own = keep(group) * keep(group) + (valid(group - 1) + valid(group + 1)) / 9.0
    c_pair = (keep(group) + keep(group + s)) * third
    c_ahead = valid(group + 2 * s) / 9.0
    c_behind = valid(group - 2 * s) / 9.0
    c_next = (keep(group + s) + keep(group + 2 * s)) * third * valid(group + 2 * s)

    sent = []

    def go(copy):
        copy.start()
        sent.append(copy)
        return copy

    pair, row, u, tx, ty = {}, {}, {}, {}, {}
    core_copy, z_copy, y_copy, gy, gz, gc = {}, {}, {}, {}, {}, {}

    def send_tx(k, d):
        c = cols(k, CHUNK)
        tx[k, d] = go(remote(
            t_own.at[:, c], t_side.at[d, :, c], tx_s.at[d, k], tx_r.at[d, k], behind if d == 0 else ahead
        ))

    def outputs(p, k):
        weights = p_own if p == 0 else params_next
        for half in range(CORES):
            c = cols(k * CORES + half, HALF)
            part = jnp.dot(h_own[...], weights[:, c], preferred_element_type=F32)
            core_keep[p, k, half] = part
            core_out[p, k, half] = part.astype(BF16)
        core_copy[p, k] = go(remote(
            core_out.at[p, k, 1 - core], core_in.at[p, k], core_s.at[p, k], core_r.at[p, k], partner
        ))

    def across_ring(p, k):
        core_copy[p, k].wait_recv()
        z_out[p, k] = (core_keep[p, k, core] + core_in[p, k].astype(F32)).astype(BF16)
        for j in range(RING - 1):
            part = pl.ds(pl.multiple_of(ring_at[j] * strip, strip), strip)
            z_copy[p, k, j] = go(remote(
                z_out.at[p, k, part], z_in.at[p, k, j], z_s.at[p, k, j], z_r.at[p, k, j], ring_peer[j]
            ))

    def across_run(p, k):
        total = z_out[p, k, ring_rows].astype(F32)
        for j in range(RING - 1):
            z_copy[p, k, j].wait_recv()
            total += z_in[p, k, j].astype(F32)
        y_out[p, k] = total.astype(BF16)
        for j in range(RUN - 1):
            part = pl.ds(pl.multiple_of(run_at[j] * PIECE, PIECE), PIECE)
            y_copy[p, k, j] = go(remote(
                y_out.at[p, k, :, part], y_in.at[p, k, j], y_s.at[p, k, j], y_r.at[p, k, j], run_peer[j]
            ))

    own_piece = pl.ds(pl.multiple_of(run * PIECE, PIECE), PIECE)

    def residual(p, k):
        total = y_out[p, k, :, own_piece].astype(F32)
        for j in range(RUN - 1):
            y_copy[p, k, j].wait_recv()
            total += y_in[p, k, j].astype(F32)
        resid = jnp.tanh(total - tgt[k].astype(F32))
        if p == 0:
            resid_old[k] = resid
            return
        gather_own[k, ring_rows, own_piece] = (resid - resid_old[k]).astype(BF16)
        block = gather_own.at[k, ring_rows, own_piece]
        for j in range(RUN - 1):
            gy[k, j] = go(remote(block, block, gy_s.at[k, j], gy_r.at[k, j], run_peer[j]))

    def back_ring(k):
        for j in range(RUN - 1):
            gy[k, j].wait_recv()
        block = gather_own.at[k, ring_rows]
        for j in range(RING - 1):
            gz[k, j] = go(remote(block, block, gz_s.at[k, j], gz_r.at[k, j], ring_peer[j]))

    def back_core(k):
        for j in range(RING - 1):
            gz[k, j].wait_recv()
        gc[k] = go(remote(gather_own.at[k], gather_other.at[k], gc_s.at[k], gc_r.at[k], partner))
        c = pl.ds(pl.multiple_of(k * CHUNK + core * HALF, HALF), HALF)
        grad[:, c] = jnp.dot(h_turned[...], gather_own[k], preferred_element_type=F32)

    def last_grad(k):
        gc[k].wait_recv()
        c = pl.ds(pl.multiple_of(k * CHUNK + (1 - core) * HALF, HALF), HALF)
        grad[:, c] = jnp.dot(h_turned[...], gather_other[k], preferred_element_type=F32)

    def send_u(k):
        c = cols(k, CHUNK)
        pair[k].wait_recv()
        u_out[:, c] = (c_ahead * p_own[:, c].astype(F32) + c_next * p_across[:, c].astype(F32)).astype(BF16)
        u[k] = go(remote(u_out.at[:, c], u_in.at[:, c], u_s.at[k], u_r.at[k], ahead))

    def send_pair(k):
        c = cols(k, CHUNK)
        block = p_own
        if k >= RAW:
            row[k].wait_recv()
            block = u_out
            u_out[:, c] = (c_pair * p_own[:, c].astype(F32) + c_next * p_side[:, c].astype(F32)).astype(BF16)
        pair[k] = go(remote(block.at[:, c], p_across.at[:, c], pair_s.at[k], pair_r.at[k], across))

    def new_params(k):
        c = cols(k, CHUNK)
        mixed = c_own * p_own[:, c].astype(F32) - step_size * t_own[:, c].astype(F32)
        u[k].wait_recv()
        if k < RAW:
            row[k].wait_recv()
            mixed += c_pair * p_across[:, c].astype(F32) + u_in[:, c].astype(F32)
        else:
            pair[k].wait_recv()
            mixed += p_across[:, c].astype(F32) + c_behind * u_in[:, c].astype(F32)
        params_next[:, c] = (mixed + c_ahead * p_side[:, c].astype(F32)).astype(BF16)

    seen = set()

    def send_ty(b):
        k = b * HALF // CHUNK
        if k not in seen:
            tx[k, 0].wait_recv()
            seen.add(k)
        c = cols(b, HALF)
        w_out[:, c] = (c_pair * t_own[:, c].astype(F32) + c_next * t_side[0, :, c].astype(F32)).astype(BF16)
        ty[b] = go(remote(w_out.at[:, c], w_in.at[:, c], ty_s.at[b], ty_r.at[b], across))

    def new_tracker(b):
        c = cols(b, HALF)
        ty[b].wait_recv()
        mixed = c_own * t_own[:, c].astype(F32) + c_ahead * t_side[0, :, c].astype(F32)
        mixed += c_behind * t_side[1, :, c].astype(F32) + w_in[:, c].astype(F32)
        tracker_next[:, c] = (mixed + grad[:, c] * (1.0 / tokens)).astype(BF16)

    loads[0].wait()
    pl.semaphore_wait(barrier, len(peers))
    for k in range(RAW):
        send_pair(k)
    for k in range(steps):
        c = cols(k, CHUNK)
        row[k] = go(remote(p_own.at[:, c], p_side.at[:, c], row_s.at[k], row_r.at[k], behind))
    for k in range(RAW, steps):
        c = cols(k, CHUNK)
        u[k] = go(remote(p_own.at[:, c], u_in.at[:, c], u_s.at[k], u_r.at[k], ahead))
    loads[1].wait()
    for k in range(steps):
        send_tx(k, 0)
    for load in loads[2:]:
        load.wait()
    h_own[...] = h_turned[...].astype(F32).T.astype(BF16)
    def side_wait():
        for k in range(steps):
            tx[k, 1].wait_recv()

    plan = [
        *[(outputs, 0, k) for k in range(steps)],
        *[(across_ring, 0, k) for k in range(steps)],
        (send_u, 0),
        *[(across_run, 0, k) for k in range(steps)],
        (send_pair, 2),
        (new_params, 0),
        (outputs, 1, 0),
        (across_ring, 1, 0),
        (send_pair, 3),
        (send_u, 1),
        *[(send_tx, k, 1) for k in range(steps)],
        (across_run, 1, 0),
        (new_params, 1),
        (outputs, 1, 1),
        (across_ring, 1, 1),
        (send_ty, 0),
        (send_ty, 1),
        (new_params, 2),
        (outputs, 1, 2),
        (across_ring, 1, 2),
        (across_run, 1, 1),
        (send_ty, 2),
        (new_params, 3),
        (outputs, 1, 3),
        (across_ring, 1, 3),
        (across_run, 1, 2),
        (across_run, 1, 3),
        *[(residual, 0, k) for k in range(steps)],
        *[(residual, 1, k) for k in range(steps)],
        *[(back_ring, k) for k in range(steps - 1)],
        *[(send_ty, b) for b in range(3, blocks)],
        (back_ring, 3),
        (side_wait,),
        (back_core, 0),
        (back_core, 1),
        (last_grad, 0),
        (back_core, 2),
        (last_grad, 1),
        (back_core, 3),
        (last_grad, 2),
        (last_grad, 3),
        *[(new_tracker, b) for b in range(blocks)],
    ]
    for step, *call in plan:
        if SCOPES:
            with jax.named_scope("_".join([step.__name__, *map(str, call)])):
                step(*call)
        else:
            step(*call)
    for copy in sent:
        copy.wait_send()


def store_kernel(params_near, tracker_near, params_far, tracker_far, sem):
    copies = [
        pltpu.make_async_copy(params_near, params_far, sem.at[0]),
        pltpu.make_async_copy(tracker_near, tracker_far, sem.at[1]),
    ]
    for copy in copies:
        copy.start()
    for copy in copies:
        copy.wait()


def body(params, tracker, hidden, target):
    _, rows, width = params.shape
    tokens = hidden.shape[0]
    steps, blocks = width // CHUNK, width // HALF
    strip = tokens // RING
    any_ = pl.BlockSpec(memory_space=pl.ANY)
    dma = pltpu.SemaphoreType.DMA
    whole = pltpu.VMEM((rows, width), BF16)
    scratch = [
        whole, whole, pltpu.VMEM(hidden.shape, BF16), pltpu.VMEM((steps, strip, PIECE), BF16),
        pltpu.VMEM((rows, tokens), BF16),
        whole, whole, whole, whole,
        pltpu.VMEM((2, rows, width), BF16), whole, whole,
        pltpu.VMEM((rows, width), F32),
        pltpu.VMEM((2, steps, CORES, tokens, HALF), BF16), pltpu.VMEM((2, steps, CORES, tokens, HALF), F32),
        pltpu.VMEM((2, steps, tokens, HALF), BF16), pltpu.VMEM((2, steps, tokens, HALF), BF16),
        pltpu.VMEM((2, steps, RING - 1, strip, HALF), BF16),
        pltpu.VMEM((2, steps, strip, HALF), BF16), pltpu.VMEM((2, steps, RUN - 1, strip, PIECE), BF16),
        pltpu.VMEM((steps, strip, PIECE), F32),
        pltpu.VMEM((steps, tokens, HALF), BF16), pltpu.VMEM((steps, tokens, HALF), BF16),
        dma((3 + steps,)),
    ]
    for shape in (
        (steps,), (steps,), (steps,), (2, steps), (blocks,),
        (2, steps), (2, steps, RING - 1), (2, steps, RUN - 1),
        (steps, RUN - 1), (steps, RING - 1), (steps,),
    ):
        scratch += [dma(shape), dma(shape)]
    near = pltpu.VMEM((rows, width), BF16)
    params_next, tracker_next = pl.pallas_call(
        step_kernel,
        out_shape=(near, near),
        in_specs=[any_] * 4,
        out_specs=[pl.BlockSpec(memory_space=pltpu.VMEM)] * 2,
        scratch_shapes=scratch,
        name="tracking_step",
        compiler_params=pltpu.CompilerParams(collective_id=0, has_side_effects=True, vmem_limit_bytes=59 << 20),
    )(params[0], tracker[0], hidden.T, target)
    far = jax.ShapeDtypeStruct((rows, width), BF16)
    params_next, tracker_next = pl.pallas_call(
        store_kernel,
        out_shape=(far, far),
        in_specs=[any_] * 2,
        out_specs=(any_, any_),
        scratch_shapes=[dma((2,))],
        name="store",
        compiler_params=pltpu.CompilerParams(vmem_limit_bytes=1 << 20),
    )(params_next, tracker_next)
    return params_next[None], tracker_next[None]


def solution(mesh):
    placed = (P("grp", "blk", None), P("grp", "blk", None), P("grp", "blk"), P("grp", None))
    return jax.shard_map(
        body,
        mesh=mesh,
        in_specs=placed,
        out_specs=(P("grp", "blk", None), P("grp", "blk", None)),
        check_vma=False,
    )
```

```python
import jax
import jax.numpy as jnp
from jax import lax
from jax.experimental import pallas as pl
from jax.experimental.pallas import tpu as pltpu
from jax.sharding import PartitionSpec as P

step_size = 0.05
MESH = pl.DeviceIdType.MESH
F32 = jnp.float32
BF16 = jnp.bfloat16

RUN = 4
RING = 8
CORES = 2
SCOPES = False
BLOCK = 256
RAW = 2
CHUNK = 1024
HALF = CHUNK // CORES
PIECE = HALF // RUN


def step_kernel(
    params, tracker, hidden, target,
    params_next, tracker_next,
    p_own, t_own, h_own, tgt, h_turned,
    p_across, p_side, u_out, u_in,
    t_side, w_out, w_in,
    grad,
    core_out, core_keep, core_in, z_out, z_in, y_out, y_in, resid_old,
    gather_own, gather_other,
    in_sem,
    pair_r, row_r, u_r, tx_r, ty_r, core_r, z_r, y_r, gy_r, gz_r, gc_r,
    pair_s, row_s, u_s, tx_s, ty_s, core_s, z_s, y_s, gy_s, gz_s, gc_s,
):
    rows, width = p_own.shape
    tokens = h_own.shape[0]
    strip = tokens // RING
    steps = width // CHUNK
    blocks = width // BLOCK
    group, place = lax.axis_index("grp"), lax.axis_index("blk")
    n_grp = lax.axis_size("grp")
    columns = n_grp // 2
    x, side = group // 2, lax.rem(group, 2)
    run, rest = place // (RING * CORES), lax.rem(place, RING * CORES)
    ring, core = rest // CORES, lax.rem(rest, CORES)
    s = 1 - 2 * side

    def at_blk(run_, ring_, core_):
        return (group, (run_ * RING + ring_) * CORES + core_)

    partner = at_blk(run, ring, 1 - core)
    ring_peer = [at_blk(run, lax.rem(ring + j, RING), core) for j in range(1, RING)]
    ring_at = [lax.rem(ring + j, RING) for j in range(1, RING)]
    run_peer = [at_blk(lax.rem(run + j, RUN), ring, core) for j in range(1, RUN)]
    run_at = [lax.rem(run + j, RUN) for j in range(1, RUN)]
    across = (x * 2 + (1 - side), place)
    ahead = (lax.rem(x + s + columns, columns) * 2 + side, place)
    behind = (lax.rem(x - s + columns, columns) * 2 + side, place)

    barrier = pltpu.get_barrier_semaphore()
    peers = [across, ahead, behind, partner] + run_peer + ring_peer
    for peer in peers:
        pl.semaphore_signal(barrier, inc=1, device_id=peer, device_id_type=MESH)

    def piece_column(k):
        return pl.multiple_of(k * CHUNK + core * HALF + run * PIECE, PIECE)

    ring_rows = pl.ds(pl.multiple_of(ring * strip, strip), strip)
    loads = [
        pltpu.make_async_copy(params, p_own, in_sem.at[0]),
        pltpu.make_async_copy(tracker, t_own, in_sem.at[1]),
        pltpu.make_async_copy(hidden, h_turned, in_sem.at[2]),
    ] + [
        pltpu.make_async_copy(
            target.at[ring_rows, pl.ds(piece_column(k), PIECE)], tgt.at[k], in_sem.at[3]
        )
        for k in range(steps)
    ]
    for load in loads:
        load.start()

    def remote(src, dst, send, recv, peer):
        return pltpu.make_async_remote_copy(
            src_ref=src, dst_ref=dst, send_sem=send, recv_sem=recv, device_id=peer, device_id_type=MESH
        )

    def cols(k, w):
        return pl.ds(k * w, w)

    def valid(i):
        return jnp.where((i >= 0) & (i < n_grp), 1.0, 0.0).astype(F32)

    def keep(i):
        return 1.0 - (valid(i - 1) + valid(i + 1)) / 3.0

    third = 1.0 / 3.0
    c_own = keep(group) * keep(group) + (valid(group - 1) + valid(group + 1)) / 9.0
    c_pair = (keep(group) + keep(group + s)) * third
    c_ahead = valid(group + 2 * s) / 9.0
    c_behind = valid(group - 2 * s) / 9.0
    c_next = (keep(group + s) + keep(group + 2 * s)) * third * valid(group + 2 * s)

    def go(copy):
        copy.start()
        return copy

    def all_of(ref, sem):
        pltpu.make_async_copy(ref, ref, sem).wait()

    pair, row, u, tx, ty = {}, {}, {}, {}, {}
    core_copy, gc = {}, {}

    def send_tx(k, d):
        c = cols(k, CHUNK)
        tx[k, d] = go(remote(
            t_own.at[:, c], t_side.at[d, :, c], tx_s, tx_r.at[k if d == 0 else steps], behind if d == 0 else ahead
        ))

    def outputs(p, k):
        weights = p_own if p == 0 else params_next
        for half in range(CORES):
            c = cols(k * CORES + half, HALF)
            part = jnp.dot(h_own[...], weights[:, c], preferred_element_type=F32)
            core_keep[p, k, half] = part
            core_out[p, k, half] = part.astype(BF16)
        core_copy[p, k] = go(remote(
            core_out.at[p, k, 1 - core], core_in.at[p, k], core_s, core_r.at[p, k], partner
        ))

    def across_ring(p, k):
        core_copy[p, k].wait_recv()
        z_out[p, k] = (core_keep[p, k, core] + core_in[p, k].astype(F32)).astype(BF16)
        for j in range(RING - 1):
            part = pl.ds(pl.multiple_of(ring_at[j] * strip, strip), strip)
            remote(z_out.at[p, k, part], z_in.at[p, k, j], z_s, z_r.at[p, k], ring_peer[j]).start()

    def across_run(p, k):
        total = z_out[p, k, ring_rows].astype(F32)
        all_of(z_in.at[p, k], z_r.at[p, k])
        for j in range(RING - 1):
            total += z_in[p, k, j].astype(F32)
        y_out[p, k] = total.astype(BF16)
        for j in range(RUN - 1):
            part = pl.ds(pl.multiple_of(run_at[j] * PIECE, PIECE), PIECE)
            remote(y_out.at[p, k, :, part], y_in.at[p, k, j], y_s, y_r.at[k if p else steps], run_peer[j]).start()

    own_piece = pl.ds(pl.multiple_of(run * PIECE, PIECE), PIECE)

    def residual(p, k):
        total = y_out[p, k, :, own_piece].astype(F32)
        if p:
            all_of(y_in.at[p, k], y_r.at[k])
        elif k == 0:
            all_of(y_in.at[p], y_r.at[steps])
        for j in range(RUN - 1):
            total += y_in[p, k, j].astype(F32)
        resid = jnp.tanh(total - tgt[k].astype(F32))
        if p == 0:
            resid_old[k] = resid
            return
        gather_own[k, ring_rows, own_piece] = (resid - resid_old[k]).astype(BF16)
        block = gather_own.at[k, ring_rows, own_piece]
        for j in range(RUN - 1):
            remote(block, block, gy_s, gy_r.at[k], run_peer[j]).start()

    def back_ring(k):
        all_of(y_in.at[1, k], gy_r.at[k])
        block = gather_own.at[k, ring_rows]
        for j in range(RING - 1):
            remote(block, block, gz_s, gz_r.at[k], ring_peer[j]).start()

    def back_core(k):
        all_of(z_in.at[1, k], gz_r.at[k])
        gc[k] = go(remote(gather_own.at[k], gather_other.at[k], gc_s, gc_r.at[k], partner))
        c = pl.ds(pl.multiple_of(k * CHUNK + core * HALF, HALF), HALF)
        grad[:, c] = jnp.dot(h_turned[...], gather_own[k], preferred_element_type=F32)

    def last_grad(k):
        gc[k].wait_recv()
        c = pl.ds(pl.multiple_of(k * CHUNK + (1 - core) * HALF, HALF), HALF)
        grad[:, c] = jnp.dot(h_turned[...], gather_other[k], preferred_element_type=F32)

    def send_u(k):
        c = cols(k, CHUNK)
        pair[k].wait_recv()
        u_out[:, c] = (c_ahead * p_own[:, c].astype(F32) + c_next * p_across[:, c].astype(F32)).astype(BF16)
        u[k] = go(remote(u_out.at[:, c], u_in.at[:, c], u_s, u_r.at[k], ahead))

    def send_pair(k):
        c = cols(k, CHUNK)
        block = p_own
        if k >= RAW:
            row[k].wait_recv()
            block = u_out
            u_out[:, c] = (c_pair * p_own[:, c].astype(F32) + c_next * p_side[:, c].astype(F32)).astype(BF16)
        pair[k] = go(remote(block.at[:, c], p_across.at[:, c], pair_s, pair_r.at[k], across))

    def new_params(k):
        c = cols(k, CHUNK)
        mixed = c_own * p_own[:, c].astype(F32) - step_size * t_own[:, c].astype(F32)
        u[k].wait_recv()
        if k < RAW:
            row[k].wait_recv()
            mixed += c_pair * p_across[:, c].astype(F32) + u_in[:, c].astype(F32)
        else:
            pair[k].wait_recv()
            mixed += p_across[:, c].astype(F32) + c_behind * u_in[:, c].astype(F32)
        params_next[:, c] = (mixed + c_ahead * p_side[:, c].astype(F32)).astype(BF16)

    seen = set()

    def send_ty(first, last):
        for b in range(first, last):
            k = b * BLOCK // CHUNK
            if k not in seen:
                tx[k, 0].wait_recv()
                seen.add(k)
            c = cols(b, BLOCK)
            w_out[:, c] = (c_pair * t_own[:, c].astype(F32) + c_next * t_side[0, :, c].astype(F32)).astype(BF16)
            ty[b] = go(remote(w_out.at[:, c], w_in.at[:, c], ty_s, ty_r.at[b], across))

    def new_tracker(b):
        c = cols(b, BLOCK)
        ty[b].wait_recv()
        mixed = c_own * t_own[:, c].astype(F32) + c_ahead * t_side[0, :, c].astype(F32)
        mixed += c_behind * t_side[1, :, c].astype(F32) + w_in[:, c].astype(F32)
        tracker_next[:, c] = (mixed + grad[:, c] * (1.0 / tokens)).astype(BF16)

    def drain():
        for ref, sem in (
            (p_own, pair_s), (p_own, row_s), (p_own, u_s), (t_side, tx_s),
            (core_in, core_s), (z_in, z_s), (y_in, y_s), (y_in.at[1], gy_s), (z_in.at[1], gz_s), (gather_own, gc_s),
        ):
            all_of(ref, sem)

    loads[0].wait()
    pl.semaphore_wait(barrier, len(peers))
    for k in range(RAW):
        send_pair(k)
    for k in range(steps):
        c = cols(k, CHUNK)
        row[k] = go(remote(p_own.at[:, c], p_side.at[:, c], row_s, row_r.at[k], behind))
    for k in range(RAW, steps):
        c = cols(k, CHUNK)
        u[k] = go(remote(p_own.at[:, c], u_in.at[:, c], u_s, u_r.at[k], ahead))
    loads[1].wait()
    for k in range(steps):
        send_tx(k, 0)
    loads[2].wait()
    all_of(tgt, in_sem.at[3])
    h_own[...] = h_turned[...].astype(F32).T.astype(BF16)
    def side_wait():
        all_of(t_side.at[1], tx_r.at[steps])

    plan = [
        *[(outputs, 0, k) for k in range(steps)],
        *[(across_ring, 0, k) for k in range(steps)],
        (send_u, 0),
        *[(across_run, 0, k) for k in range(steps)],
        (send_pair, 2),
        (new_params, 0),
        (outputs, 1, 0),
        (across_ring, 1, 0),
        (send_pair, 3),
        (send_u, 1),
        *[(send_tx, k, 1) for k in range(steps)],
        (across_run, 1, 0),
        (new_params, 1),
        (outputs, 1, 1),
        (across_ring, 1, 1),
        (send_ty, 0, 4),
        (new_params, 2),
        (outputs, 1, 2),
        (across_ring, 1, 2),
        (across_run, 1, 1),
        (send_ty, 4, 6),
        (new_params, 3),
        (outputs, 1, 3),
        (across_ring, 1, 3),
        (across_run, 1, 2),
        (across_run, 1, 3),
        (send_ty, 6, 7),
        *[(residual, 0, k) for k in range(steps)],
        *[(residual, 1, k) for k in range(steps)],
        *[(back_ring, k) for k in range(steps - 1)],
        (send_ty, 7, blocks),
        (back_ring, 3),
        (side_wait,),
        (back_core, 0),
        (back_core, 1),
        (last_grad, 0),
        (back_core, 2),
        (last_grad, 1),
        (back_core, 3),
        (last_grad, 2),
        (last_grad, 3),
        (drain,),
        *[(new_tracker, b) for b in range(blocks)],
    ]
    for step, *call in plan:
        if SCOPES:
            with jax.named_scope("_".join([step.__name__, *map(str, call)])):
                step(*call)
        else:
            step(*call)
    all_of(w_out, ty_s)


def store_kernel(params_near, tracker_near, params_far, tracker_far, sem):
    copies = [
        pltpu.make_async_copy(params_near, params_far, sem.at[0]),
        pltpu.make_async_copy(tracker_near, tracker_far, sem.at[1]),
    ]
    for copy in copies:
        copy.start()
    for copy in copies:
        copy.wait()


def body(params, tracker, hidden, target):
    _, rows, width = params.shape
    tokens = hidden.shape[0]
    steps, blocks = width // CHUNK, width // BLOCK
    strip = tokens // RING
    any_ = pl.BlockSpec(memory_space=pl.ANY)
    dma = pltpu.SemaphoreType.DMA
    whole = pltpu.VMEM((rows, width), BF16)
    scratch = [
        whole, whole, pltpu.VMEM(hidden.shape, BF16), pltpu.VMEM((steps, strip, PIECE), BF16),
        pltpu.VMEM((rows, tokens), BF16),
        whole, whole, whole, whole,
        pltpu.VMEM((2, rows, width), BF16), whole, whole,
        pltpu.VMEM((rows, width), F32),
        pltpu.VMEM((2, steps, CORES, tokens, HALF), BF16), pltpu.VMEM((2, steps, CORES, tokens, HALF), F32),
        pltpu.VMEM((2, steps, tokens, HALF), BF16), pltpu.VMEM((2, steps, tokens, HALF), BF16),
        pltpu.VMEM((2, steps, RING - 1, strip, HALF), BF16),
        pltpu.VMEM((2, steps, strip, HALF), BF16), pltpu.VMEM((2, steps, RUN - 1, strip, PIECE), BF16),
        pltpu.VMEM((steps, strip, PIECE), F32),
        pltpu.VMEM((steps, tokens, HALF), BF16), pltpu.VMEM((steps, tokens, HALF), BF16),
        dma((4,)),
    ]
    scratch += [dma((steps,)), dma((steps,)), dma((steps,)), dma((steps + 1,)), dma((blocks,))]
    scratch += [dma((2, steps)), dma((2, steps)), dma((steps + 1,)), dma((steps,)), dma((steps,)), dma((steps,))]
    scratch += [dma(())] * 11
    near = pltpu.VMEM((rows, width), BF16)
    params_next, tracker_next = pl.pallas_call(
        step_kernel,
        out_shape=(near, near),
        in_specs=[any_] * 4,
        out_specs=[pl.BlockSpec(memory_space=pltpu.VMEM)] * 2,
        scratch_shapes=scratch,
        name="tracking_step",
        compiler_params=pltpu.CompilerParams(collective_id=0, has_side_effects=True, vmem_limit_bytes=59 << 20),
    )(params[0], tracker[0], hidden.T, target)
    far = jax.ShapeDtypeStruct((rows, width), BF16)
    params_next, tracker_next = pl.pallas_call(
        store_kernel,
        out_shape=(far, far),
        in_specs=[any_] * 2,
        out_specs=(any_, any_),
        scratch_shapes=[dma((2,))],
        name="store",
        compiler_params=pltpu.CompilerParams(vmem_limit_bytes=1 << 20),
    )(params_next, tracker_next)
    return params_next[None], tracker_next[None]


def solution(mesh):
    placed = (P("grp", "blk", None), P("grp", "blk", None), P("grp", "blk"), P("grp", None))
    return jax.shard_map(
        body,
        mesh=mesh,
        in_specs=placed,
        out_specs=(P("grp", "blk", None), P("grp", "blk", None)),
        check_vma=False,
    )
```

```python
import jax
import jax.numpy as jnp
from jax import lax
from jax.experimental import pallas as pl
from jax.experimental.pallas import tpu as pltpu
from jax.sharding import PartitionSpec as P

step_size = 0.05
MESH = pl.DeviceIdType.MESH
F32 = jnp.float32
BF16 = jnp.bfloat16

RUN = 4
RING = 8
CORES = 2
SCOPES = False
BLOCK = 256
RAW = 2
CHUNK = 1024
HALF = CHUNK // CORES
PIECE = HALF // RUN


def step_kernel(
    params, tracker, hidden, target,
    params_next, tracker_next,
    p_own, t_own, h_own, tgt, h_turned,
    p_across, p_side, u_out, u_in,
    t_side, w_out, w_in,
    grad,
    core_out, core_keep, core_in, z_out, z_in, y_out, y_in, resid_old,
    gather_own, gather_other,
    in_sem,
    pair_r, row_r, u_r, tx_r, ty_r, core_r, z_r, y_r, gy_r, gz_r, gc_r,
    pair_s, row_s, u_s, tx_s, ty_s, core_s, z_s, y_s, gy_s, gz_s, gc_s,
    met,
):
    rows, width = p_own.shape
    tokens = h_own.shape[0]
    strip = tokens // RING
    steps = width // CHUNK
    blocks = width // BLOCK
    group, place = lax.axis_index("grp"), lax.axis_index("blk")
    n_grp = lax.axis_size("grp")
    columns = n_grp // 2
    x, side = group // 2, lax.rem(group, 2)
    run, rest = place // (RING * CORES), lax.rem(place, RING * CORES)
    ring, core = rest // CORES, lax.rem(rest, CORES)
    s = 1 - 2 * side

    def at_blk(run_, ring_, core_):
        return (group, (run_ * RING + ring_) * CORES + core_)

    partner = at_blk(run, ring, 1 - core)
    ring_peer = [at_blk(run, lax.rem(ring + j, RING), core) for j in range(1, RING)]
    ring_at = [lax.rem(ring + j, RING) for j in range(1, RING)]
    run_peer = [at_blk(lax.rem(run + j, RUN), ring, core) for j in range(1, RUN)]
    run_at = [lax.rem(run + j, RUN) for j in range(1, RUN)]
    across = (x * 2 + (1 - side), place)
    ahead = (lax.rem(x + s + columns, columns) * 2 + side, place)
    behind = (lax.rem(x - s + columns, columns) * 2 + side, place)

    barrier = pltpu.get_barrier_semaphore()
    peers = [across, ahead, behind, partner] + run_peer
    for peer in peers:
        pl.semaphore_signal(barrier, inc=1, device_id=peer, device_id_type=MESH)

    def greet(sem, j):
        pl.semaphore_signal(sem, inc=1, device_id=ring_peer[j], device_id_type=MESH)

    for j in range(RING - 1):
        pl.when(ring_at[j] > ring)(lambda: greet(barrier, j))

    def piece_column(k):
        return pl.multiple_of(k * CHUNK + core * HALF + run * PIECE, PIECE)

    ring_rows = pl.ds(pl.multiple_of(ring * strip, strip), strip)
    loads = [
        pltpu.make_async_copy(params, p_own, in_sem.at[0]),
        pltpu.make_async_copy(tracker, t_own, in_sem.at[1]),
        pltpu.make_async_copy(hidden, h_turned, in_sem.at[2]),
    ] + [
        pltpu.make_async_copy(
            target.at[ring_rows, pl.ds(piece_column(k), PIECE)], tgt.at[k], in_sem.at[3]
        )
        for k in range(steps)
    ]
    for load in loads:
        load.start()

    def remote(src, dst, send, recv, peer):
        return pltpu.make_async_remote_copy(
            src_ref=src, dst_ref=dst, send_sem=send, recv_sem=recv, device_id=peer, device_id_type=MESH
        )

    def cols(k, w):
        return pl.ds(k * w, w)

    def valid(i):
        return jnp.where((i >= 0) & (i < n_grp), 1.0, 0.0).astype(F32)

    def keep(i):
        return 1.0 - (valid(i - 1) + valid(i + 1)) / 3.0

    third = 1.0 / 3.0
    c_own = keep(group) * keep(group) + (valid(group - 1) + valid(group + 1)) / 9.0
    c_pair = (keep(group) + keep(group + s)) * third
    c_ahead = valid(group + 2 * s) / 9.0
    c_behind = valid(group - 2 * s) / 9.0
    c_next = (keep(group + s) + keep(group + 2 * s)) * third * valid(group + 2 * s)

    def go(copy):
        copy.start()
        return copy

    def all_of(ref, sem):
        pltpu.make_async_copy(ref, ref, sem).wait()

    pair, row, u, tx, ty = {}, {}, {}, {}, {}
    core_copy, gc = {}, {}

    def send_tx(k, d):
        c = cols(k, CHUNK)
        tx[k, d] = go(remote(
            t_own.at[:, c], t_side.at[d, :, c], tx_s, tx_r.at[k if d == 0 else steps], behind if d == 0 else ahead
        ))

    def outputs(p, k):
        weights = p_own if p == 0 else params_next
        for half in range(CORES):
            c = cols(k * CORES + half, HALF)
            part = jnp.dot(h_own[...], weights[:, c], preferred_element_type=F32)
            core_keep[p, k, half] = part
            core_out[p, k, half] = part.astype(BF16)
        core_copy[p, k] = go(remote(
            core_out.at[p, k, 1 - core], core_in.at[p, k], core_s, core_r.at[p, k], partner
        ))

    def ring_met():
        @pl.when(ring < RING - 1)
        def _():
            pl.semaphore_wait(met, RING - 1 - ring)

    def across_ring(p, k):
        core_copy[p, k].wait_recv()
        z_out[p, k] = (core_keep[p, k, core] + core_in[p, k].astype(F32)).astype(BF16)
        for j in range(RING - 1):
            part = pl.ds(pl.multiple_of(ring_at[j] * strip, strip), strip)
            remote(z_out.at[p, k, part], z_in.at[p, k, j], z_s, z_r.at[p, k], ring_peer[j]).start()

    def across_run(p, k):
        total = z_out[p, k, ring_rows].astype(F32)
        all_of(z_in.at[p, k], z_r.at[p, k])
        for j in range(RING - 1):
            total += z_in[p, k, j].astype(F32)
        y_out[p, k] = total.astype(BF16)
        for j in range(RUN - 1):
            part = pl.ds(pl.multiple_of(run_at[j] * PIECE, PIECE), PIECE)
            remote(y_out.at[p, k, :, part], y_in.at[p, k, j], y_s, y_r.at[k if p else steps], run_peer[j]).start()

    own_piece = pl.ds(pl.multiple_of(run * PIECE, PIECE), PIECE)

    def residual(p, k):
        total = y_out[p, k, :, own_piece].astype(F32)
        if p:
            all_of(y_in.at[p, k], y_r.at[k])
        elif k == 0:
            all_of(y_in.at[p], y_r.at[steps])
        for j in range(RUN - 1):
            total += y_in[p, k, j].astype(F32)
        resid = jnp.tanh(total - tgt[k].astype(F32))
        if p == 0:
            resid_old[k] = resid
            return
        gather_own[k, ring_rows, own_piece] = (resid - resid_old[k]).astype(BF16)
        block = gather_own.at[k, ring_rows, own_piece]
        for j in range(RUN - 1):
            remote(block, block, gy_s, gy_r.at[k], run_peer[j]).start()

    def back_ring(k):
        all_of(y_in.at[1, k], gy_r.at[k])
        block = gather_own.at[k, ring_rows]
        for j in range(RING - 1):
            remote(block, block, gz_s, gz_r.at[k], ring_peer[j]).start()

    def back_core(k):
        all_of(z_in.at[1, k], gz_r.at[k])
        gc[k] = go(remote(gather_own.at[k], gather_other.at[k], gc_s, gc_r.at[k], partner))
        c = pl.ds(pl.multiple_of(k * CHUNK + core * HALF, HALF), HALF)
        grad[:, c] = jnp.dot(h_turned[...], gather_own[k], preferred_element_type=F32)

    def last_grad(k):
        gc[k].wait_recv()
        c = pl.ds(pl.multiple_of(k * CHUNK + (1 - core) * HALF, HALF), HALF)
        grad[:, c] = jnp.dot(h_turned[...], gather_other[k], preferred_element_type=F32)

    def send_u(k):
        c = cols(k, CHUNK)
        pair[k].wait_recv()
        u_out[:, c] = (c_ahead * p_own[:, c].astype(F32) + c_next * p_across[:, c].astype(F32)).astype(BF16)
        u[k] = go(remote(u_out.at[:, c], u_in.at[:, c], u_s, u_r.at[k], ahead))

    def send_pair(k):
        c = cols(k, CHUNK)
        block = p_own
        if k >= RAW:
            row[k].wait_recv()
            block = u_out
            u_out[:, c] = (c_pair * p_own[:, c].astype(F32) + c_next * p_side[:, c].astype(F32)).astype(BF16)
        pair[k] = go(remote(block.at[:, c], p_across.at[:, c], pair_s, pair_r.at[k], across))

    def new_params(k):
        c = cols(k, CHUNK)
        mixed = c_own * p_own[:, c].astype(F32) - step_size * t_own[:, c].astype(F32)
        u[k].wait_recv()
        if k < RAW:
            row[k].wait_recv()
            mixed += c_pair * p_across[:, c].astype(F32) + u_in[:, c].astype(F32)
        else:
            pair[k].wait_recv()
            mixed += p_across[:, c].astype(F32) + c_behind * u_in[:, c].astype(F32)
        params_next[:, c] = (mixed + c_ahead * p_side[:, c].astype(F32)).astype(BF16)

    seen = set()

    def send_ty(first, last):
        for b in range(first, last):
            k = b * BLOCK // CHUNK
            if k not in seen:
                tx[k, 0].wait_recv()
                seen.add(k)
            c = cols(b, BLOCK)
            w_out[:, c] = (c_pair * t_own[:, c].astype(F32) + c_next * t_side[0, :, c].astype(F32)).astype(BF16)
            ty[b] = go(remote(w_out.at[:, c], w_in.at[:, c], ty_s, ty_r.at[b], across))

    def new_tracker(b):
        c = cols(b, BLOCK)
        ty[b].wait_recv()
        mixed = c_own * t_own[:, c].astype(F32) + c_ahead * t_side[0, :, c].astype(F32)
        mixed += c_behind * t_side[1, :, c].astype(F32) + w_in[:, c].astype(F32)
        tracker_next[:, c] = (mixed + grad[:, c] * (1.0 / tokens)).astype(BF16)

    def drain():
        for ref, sem in (
            (p_own, pair_s), (p_own, row_s), (p_own, u_s), (t_side, tx_s),
            (core_in, core_s), (z_in, z_s), (y_in, y_s), (y_in.at[1], gy_s), (z_in.at[1], gz_s), (gather_own, gc_s),
        ):
            all_of(ref, sem)

    loads[0].wait()
    pl.semaphore_wait(barrier, len(peers) + ring)
    for j in range(RING - 1):
        pl.when(ring_at[j] < ring)(lambda: greet(met, j))
    for k in range(RAW):
        send_pair(k)
    for k in range(steps):
        c = cols(k, CHUNK)
        row[k] = go(remote(p_own.at[:, c], p_side.at[:, c], row_s, row_r.at[k], behind))
    for k in range(RAW, steps):
        c = cols(k, CHUNK)
        u[k] = go(remote(p_own.at[:, c], u_in.at[:, c], u_s, u_r.at[k], ahead))
    loads[1].wait()
    for k in range(steps):
        send_tx(k, 0)
    loads[2].wait()
    all_of(tgt, in_sem.at[3])
    h_own[...] = h_turned[...].astype(F32).T.astype(BF16)
    def side_wait():
        all_of(t_side.at[1], tx_r.at[steps])

    plan = [
        *[(outputs, 0, k) for k in range(steps)],
        (ring_met,),
        *[(across_ring, 0, k) for k in range(steps)],
        (send_u, 0),
        (send_pair, 2),
        (new_params, 0),
        (outputs, 1, 0),
        (send_pair, 3),
        *[(across_run, 0, k) for k in range(steps)],
        (across_ring, 1, 0),
        (send_u, 1),
        *[(send_tx, k, 1) for k in range(steps)],
        (across_run, 1, 0),
        (new_params, 1),
        (outputs, 1, 1),
        (send_ty, 0, 4),
        (across_ring, 1, 1),
        (new_params, 2),
        (outputs, 1, 2),
        (across_ring, 1, 2),
        (send_ty, 4, 7),
        (across_run, 1, 1),
        (new_params, 3),
        (outputs, 1, 3),
        (across_ring, 1, 3),
        (across_run, 1, 2),
        (across_run, 1, 3),
        (send_ty, 7, 8),
        *[(residual, 0, k) for k in range(steps)],
        *[(residual, 1, k) for k in range(steps)],
        (back_ring, 0),
        (back_ring, 1),
        (back_ring, 2),
        (send_ty, 8, blocks),
        (back_ring, 3),
        (side_wait,),
        (back_core, 0),
        (back_core, 1),
        (last_grad, 0),
        (back_core, 2),
        (last_grad, 1),
        (back_core, 3),
        (last_grad, 2),
        (last_grad, 3),
        (drain,),
        *[(new_tracker, b) for b in range(blocks)],
    ]
    for step, *call in plan:
        if SCOPES:
            with jax.named_scope("_".join([step.__name__, *map(str, call)])):
                step(*call)
        else:
            step(*call)
    all_of(w_out, ty_s)


def store_kernel(params_near, tracker_near, params_far, tracker_far, sem):
    copies = [
        pltpu.make_async_copy(params_near, params_far, sem.at[0]),
        pltpu.make_async_copy(tracker_near, tracker_far, sem.at[1]),
    ]
    for copy in copies:
        copy.start()
    for copy in copies:
        copy.wait()


def body(params, tracker, hidden, target):
    _, rows, width = params.shape
    tokens = hidden.shape[0]
    steps, blocks = width // CHUNK, width // BLOCK
    strip = tokens // RING
    any_ = pl.BlockSpec(memory_space=pl.ANY)
    dma = pltpu.SemaphoreType.DMA
    whole = pltpu.VMEM((rows, width), BF16)
    scratch = [
        whole, whole, pltpu.VMEM(hidden.shape, BF16), pltpu.VMEM((steps, strip, PIECE), BF16),
        pltpu.VMEM((rows, tokens), BF16),
        whole, whole, whole, whole,
        pltpu.VMEM((2, rows, width), BF16), whole, whole,
        pltpu.VMEM((rows, width), F32),
        pltpu.VMEM((2, steps, CORES, tokens, HALF), BF16), pltpu.VMEM((2, steps, CORES, tokens, HALF), F32),
        pltpu.VMEM((2, steps, tokens, HALF), BF16), pltpu.VMEM((2, steps, tokens, HALF), BF16),
        pltpu.VMEM((2, steps, RING - 1, strip, HALF), BF16),
        pltpu.VMEM((2, steps, strip, HALF), BF16), pltpu.VMEM((2, steps, RUN - 1, strip, PIECE), BF16),
        pltpu.VMEM((steps, strip, PIECE), F32),
        pltpu.VMEM((steps, tokens, HALF), BF16), pltpu.VMEM((steps, tokens, HALF), BF16),
        dma((4,)),
    ]
    scratch += [dma((steps,)), dma((steps,)), dma((steps,)), dma((steps + 1,)), dma((blocks,))]
    scratch += [dma((2, steps)), dma((2, steps)), dma((steps + 1,)), dma((steps,)), dma((steps,)), dma((steps,))]
    scratch += [dma(())] * 11 + [pltpu.SemaphoreType.REGULAR]
    near = pltpu.VMEM((rows, width), BF16)
    params_next, tracker_next = pl.pallas_call(
        step_kernel,
        out_shape=(near, near),
        in_specs=[any_] * 4,
        out_specs=[pl.BlockSpec(memory_space=pltpu.VMEM)] * 2,
        scratch_shapes=scratch,
        name="tracking_step",
        compiler_params=pltpu.CompilerParams(collective_id=0, has_side_effects=True, vmem_limit_bytes=59 << 20),
    )(params[0], tracker[0], hidden.T, target)
    far = jax.ShapeDtypeStruct((rows, width), BF16)
    params_next, tracker_next = pl.pallas_call(
        store_kernel,
        out_shape=(far, far),
        in_specs=[any_] * 2,
        out_specs=(any_, any_),
        scratch_shapes=[dma((2,))],
        name="store",
        compiler_params=pltpu.CompilerParams(vmem_limit_bytes=1 << 20),
    )(params_next, tracker_next)
    return params_next[None], tracker_next[None]


def solution(mesh):
    placed = (P("grp", "blk", None), P("grp", "blk", None), P("grp", "blk"), P("grp", None))
    return jax.shard_map(
        body,
        mesh=mesh,
        in_specs=placed,
        out_specs=(P("grp", "blk", None), P("grp", "blk", None)),
        check_vma=False,
    )
```

```python
import jax
import jax.numpy as jnp
from jax import lax
from jax.experimental import pallas as pl
from jax.experimental.pallas import tpu as pltpu
from jax.sharding import PartitionSpec as P

step_size = 0.05
MESH = pl.DeviceIdType.MESH
F32 = jnp.float32
BF16 = jnp.bfloat16

RUN = 4
RING = 8
CORES = 2
SCOPES = False
BLOCK = 256
RAW = 2
CHUNK = 1024
HALF = CHUNK // CORES
PIECE = HALF // RUN


def step_kernel(
    params, tracker, hidden, target,
    params_next, tracker_next,
    p_own, t_own, h_own, tgt, h_turned,
    p_across, p_side, u_out, u_in,
    t_side, w_out, w_in,
    grad,
    core_out, core_keep, core_in, z_out, z_in, y_out, y_in, resid_old,
    gather_own, gather_other,
    in_sem,
    pair_r, row_r, u_r, tx_r, ty_r, core_r, z_r, y_r, gy_r, gz_r, gc_r,
    pair_s, row_s, u_s, tx_s, ty_s, core_s, z_s, y_s, gy_s, gz_s, gc_s,
    met,
):
    rows, width = p_own.shape
    tokens = h_own.shape[0]
    strip = tokens // RING
    steps = width // CHUNK
    blocks = width // BLOCK
    group, place = lax.axis_index("grp"), lax.axis_index("blk")
    n_grp = lax.axis_size("grp")
    columns = n_grp // 2
    x, side = group // 2, lax.rem(group, 2)
    run, rest = place // (RING * CORES), lax.rem(place, RING * CORES)
    ring, core = rest // CORES, lax.rem(rest, CORES)
    s = 1 - 2 * side

    def at_blk(run_, ring_, core_):
        return (group, (run_ * RING + ring_) * CORES + core_)

    partner = at_blk(run, ring, 1 - core)
    ring_peer = [at_blk(run, lax.rem(ring + j, RING), core) for j in range(1, RING)]
    ring_at = [lax.rem(ring + j, RING) for j in range(1, RING)]
    run_peer = [at_blk(lax.rem(run + j, RUN), ring, core) for j in range(1, RUN)]
    run_at = [lax.rem(run + j, RUN) for j in range(1, RUN)]
    across = (x * 2 + (1 - side), place)
    ahead = (lax.rem(x + s + columns, columns) * 2 + side, place)
    behind = (lax.rem(x - s + columns, columns) * 2 + side, place)

    barrier = pltpu.get_barrier_semaphore()
    peers = [across, ahead, behind, partner] + run_peer
    for peer in peers:
        pl.semaphore_signal(barrier, inc=1, device_id=peer, device_id_type=MESH)

    def greet(sem, j):
        pl.semaphore_signal(sem, inc=1, device_id=ring_peer[j], device_id_type=MESH)

    for j in range(RING - 1):
        pl.when(ring_at[j] > ring)(lambda: greet(barrier, j))

    def piece_column(k):
        return pl.multiple_of(k * CHUNK + core * HALF + run * PIECE, PIECE)

    ring_rows = pl.ds(pl.multiple_of(ring * strip, strip), strip)
    loads = [
        pltpu.make_async_copy(params, p_own, in_sem.at[0]),
        pltpu.make_async_copy(tracker, t_own, in_sem.at[1]),
        pltpu.make_async_copy(hidden, h_turned, in_sem.at[2]),
    ] + [
        pltpu.make_async_copy(
            target.at[ring_rows, pl.ds(piece_column(k), PIECE)], tgt.at[k], in_sem.at[3]
        )
        for k in range(steps)
    ]
    for load in loads:
        load.start()

    def remote(src, dst, send, recv, peer):
        return pltpu.make_async_remote_copy(
            src_ref=src, dst_ref=dst, send_sem=send, recv_sem=recv, device_id=peer, device_id_type=MESH
        )

    def cols(k, w):
        return pl.ds(k * w, w)

    def valid(i):
        return jnp.where((i >= 0) & (i < n_grp), 1.0, 0.0).astype(F32)

    def keep(i):
        return 1.0 - (valid(i - 1) + valid(i + 1)) / 3.0

    third = 1.0 / 3.0
    c_own = keep(group) * keep(group) + (valid(group - 1) + valid(group + 1)) / 9.0
    c_pair = (keep(group) + keep(group + s)) * third
    c_ahead = valid(group + 2 * s) / 9.0
    c_behind = valid(group - 2 * s) / 9.0
    c_next = (keep(group + s) + keep(group + 2 * s)) * third * valid(group + 2 * s)

    def go(copy):
        copy.start()
        return copy

    def all_of(ref, sem):
        pltpu.make_async_copy(ref, ref, sem).wait()

    pair, row, u, tx, ty = {}, {}, {}, {}, {}
    core_copy, gc = {}, {}

    def send_tx(k, d):
        c = cols(k, CHUNK)
        tx[k, d] = go(remote(
            t_own.at[:, c], t_side.at[d, :, c], tx_s, tx_r.at[k if d == 0 else steps], behind if d == 0 else ahead
        ))

    def outputs(p, k):
        weights = p_own if p == 0 else params_next
        for half in range(CORES):
            c = cols(k * CORES + half, HALF)
            part = jnp.dot(h_own[...], weights[:, c], preferred_element_type=F32)
            core_keep[p, k, half] = part
            core_out[p, k, half] = part.astype(BF16)
        core_copy[p, k] = go(remote(
            core_out.at[p, k, 1 - core], core_in.at[p, k], core_s, core_r.at[p, k], partner
        ))

    def ring_met():
        @pl.when(ring < RING - 1)
        def _():
            pl.semaphore_wait(met, RING - 1 - ring)

    def across_ring(p, k):
        core_copy[p, k].wait_recv()
        z_out[p, k] = (core_keep[p, k, core] + core_in[p, k].astype(F32)).astype(BF16)
        for j in range(RING - 1):
            part = pl.ds(pl.multiple_of(ring_at[j] * strip, strip), strip)
            remote(z_out.at[p, k, part], z_in.at[p, k, j], z_s, z_r.at[p, k], ring_peer[j]).start()

    def across_run(p, k):
        total = z_out[p, k, ring_rows].astype(F32)
        all_of(z_in.at[p, k], z_r.at[p, k])
        for j in range(RING - 1):
            total += z_in[p, k, j].astype(F32)
        y_out[p, k] = total.astype(BF16)
        for j in range(RUN - 1):
            part = pl.ds(pl.multiple_of(run_at[j] * PIECE, PIECE), PIECE)
            remote(y_out.at[p, k, :, part], y_in.at[p, k, j], y_s, y_r.at[k if p else steps], run_peer[j]).start()

    own_piece = pl.ds(pl.multiple_of(run * PIECE, PIECE), PIECE)

    def residual(p, k):
        total = y_out[p, k, :, own_piece].astype(F32)
        if p:
            all_of(y_in.at[p, k], y_r.at[k])
        elif k == 0:
            all_of(y_in.at[p], y_r.at[steps])
        for j in range(RUN - 1):
            total += y_in[p, k, j].astype(F32)
        resid = jnp.tanh(total - tgt[k].astype(F32))
        if p == 0:
            resid_old[k] = resid
            return
        gather_own[k, ring_rows, own_piece] = (resid - resid_old[k]).astype(BF16)
        block = gather_own.at[k, ring_rows, own_piece]
        for j in range(RUN - 1):
            remote(block, block, gy_s, gy_r.at[k], run_peer[j]).start()

    def back_ring(k):
        all_of(y_in.at[1, k], gy_r.at[k])
        block = gather_own.at[k, ring_rows]
        for j in range(RING - 1):
            remote(block, block, gz_s, gz_r.at[k], ring_peer[j]).start()

    def back_core(k):
        all_of(z_in.at[1, k], gz_r.at[k])
        gc[k] = go(remote(gather_own.at[k], gather_other.at[k], gc_s, gc_r.at[k], partner))
        c = pl.ds(pl.multiple_of(k * CHUNK + core * HALF, HALF), HALF)
        grad[:, c] = jnp.dot(h_turned[...], gather_own[k], preferred_element_type=F32)

    def last_grad(k):
        gc[k].wait_recv()
        c = pl.ds(pl.multiple_of(k * CHUNK + (1 - core) * HALF, HALF), HALF)
        grad[:, c] = jnp.dot(h_turned[...], gather_other[k], preferred_element_type=F32)

    def send_u(k):
        c = cols(k, CHUNK)
        pair[k].wait_recv()
        u_out[:, c] = (c_ahead * p_own[:, c].astype(F32) + c_next * p_across[:, c].astype(F32)).astype(BF16)
        u[k] = go(remote(u_out.at[:, c], u_in.at[:, c], u_s, u_r.at[k], ahead))

    def send_pair(k):
        c = cols(k, CHUNK)
        block = p_own
        if k >= RAW:
            row[k].wait_recv()
            block = u_out
            u_out[:, c] = (c_pair * p_own[:, c].astype(F32) + c_next * p_side[:, c].astype(F32)).astype(BF16)
        pair[k] = go(remote(block.at[:, c], p_across.at[:, c], pair_s, pair_r.at[k], across))

    def new_params(k):
        c = cols(k, CHUNK)
        mixed = c_own * p_own[:, c].astype(F32) - step_size * t_own[:, c].astype(F32)
        u[k].wait_recv()
        if k < RAW:
            row[k].wait_recv()
            mixed += c_pair * p_across[:, c].astype(F32) + u_in[:, c].astype(F32)
        else:
            pair[k].wait_recv()
            mixed += p_across[:, c].astype(F32) + c_behind * u_in[:, c].astype(F32)
        params_next[:, c] = (mixed + c_ahead * p_side[:, c].astype(F32)).astype(BF16)

    seen = set()

    def send_ty(first, last):
        for b in range(first, last):
            k = b * BLOCK // CHUNK
            if k not in seen:
                tx[k, 0].wait_recv()
                seen.add(k)
            c = cols(b, BLOCK)
            w_out[:, c] = (c_pair * t_own[:, c].astype(F32) + c_next * t_side[0, :, c].astype(F32)).astype(BF16)
            ty[b] = go(remote(w_out.at[:, c], w_in.at[:, c], ty_s, ty_r.at[b // 2], across))

    def new_tracker(b):
        c = cols(b, BLOCK)
        if b % 2 == 0:
            all_of(w_in.at[:, cols(b // 2, 2 * BLOCK)], ty_r.at[b // 2])
        mixed = c_own * t_own[:, c].astype(F32) + c_ahead * t_side[0, :, c].astype(F32)
        mixed += c_behind * t_side[1, :, c].astype(F32) + w_in[:, c].astype(F32)
        tracker_next[:, c] = (mixed + grad[:, c] * (1.0 / tokens)).astype(BF16)

    def drain():
        for ref, sem in (
            (p_own, pair_s), (p_own, row_s), (p_own, u_s), (t_side, tx_s),
            (core_in, core_s), (z_in, z_s), (y_in, y_s), (y_in.at[1], gy_s), (z_in.at[1], gz_s), (gather_own, gc_s),
        ):
            all_of(ref, sem)

    loads[0].wait()
    pl.semaphore_wait(barrier, len(peers) + ring)
    for j in range(RING - 1):
        pl.when(ring_at[j] < ring)(lambda: greet(met, j))
    for k in range(RAW):
        send_pair(k)
    for k in range(steps):
        c = cols(k, CHUNK)
        row[k] = go(remote(p_own.at[:, c], p_side.at[:, c], row_s, row_r.at[k], behind))
    for k in range(RAW, steps):
        c = cols(k, CHUNK)
        u[k] = go(remote(p_own.at[:, c], u_in.at[:, c], u_s, u_r.at[k], ahead))
    loads[1].wait()
    for k in range(steps):
        send_tx(k, 0)
    loads[2].wait()
    all_of(tgt, in_sem.at[3])
    h_own[...] = h_turned[...].astype(F32).T.astype(BF16)
    def side_wait():
        all_of(t_side.at[1], tx_r.at[steps])

    plan = [
        *[(outputs, 0, k) for k in range(steps)],
        (ring_met,),
        *[(across_ring, 0, k) for k in range(steps)],
        (send_u, 0),
        (send_pair, 2),
        (new_params, 0),
        (outputs, 1, 0),
        (send_pair, 3),
        *[(across_run, 0, k) for k in range(steps)],
        (across_ring, 1, 0),
        (send_u, 1),
        *[(send_tx, k, 1) for k in range(steps)],
        (across_run, 1, 0),
        (new_params, 1),
        (outputs, 1, 1),
        (send_ty, 0, 4),
        (across_ring, 1, 1),
        (new_params, 2),
        (outputs, 1, 2),
        (across_ring, 1, 2),
        (send_ty, 4, 7),
        (across_run, 1, 1),
        (new_params, 3),
        (outputs, 1, 3),
        (across_ring, 1, 3),
        (across_run, 1, 2),
        (across_run, 1, 3),
        (send_ty, 7, 8),
        *[(residual, 0, k) for k in range(steps)],
        *[(residual, 1, k) for k in range(steps)],
        (back_ring, 0),
        (back_ring, 1),
        (send_ty, 8, blocks),
        (back_ring, 2),
        (back_ring, 3),
        (side_wait,),
        (back_core, 0),
        (back_core, 1),
        (last_grad, 0),
        (back_core, 2),
        (last_grad, 1),
        (back_core, 3),
        (last_grad, 2),
        (last_grad, 3),
        (drain,),
        *[(new_tracker, b) for b in range(blocks)],
    ]
    for step, *call in plan:
        if SCOPES:
            with jax.named_scope("_".join([step.__name__, *map(str, call)])):
                step(*call)
        else:
            step(*call)
    all_of(w_out, ty_s)


def store_kernel(params_near, tracker_near, params_far, tracker_far, sem):
    copies = [
        pltpu.make_async_copy(params_near, params_far, sem.at[0]),
        pltpu.make_async_copy(tracker_near, tracker_far, sem.at[1]),
    ]
    for copy in copies:
        copy.start()
    for copy in copies:
        copy.wait()


def body(params, tracker, hidden, target):
    _, rows, width = params.shape
    tokens = hidden.shape[0]
    steps, blocks = width // CHUNK, width // BLOCK
    strip = tokens // RING
    any_ = pl.BlockSpec(memory_space=pl.ANY)
    dma = pltpu.SemaphoreType.DMA
    whole = pltpu.VMEM((rows, width), BF16)
    scratch = [
        whole, whole, pltpu.VMEM(hidden.shape, BF16), pltpu.VMEM((steps, strip, PIECE), BF16),
        pltpu.VMEM((rows, tokens), BF16),
        whole, whole, whole, whole,
        pltpu.VMEM((2, rows, width), BF16), whole, whole,
        pltpu.VMEM((rows, width), F32),
        pltpu.VMEM((2, steps, CORES, tokens, HALF), BF16), pltpu.VMEM((2, steps, CORES, tokens, HALF), F32),
        pltpu.VMEM((2, steps, tokens, HALF), BF16), pltpu.VMEM((2, steps, tokens, HALF), BF16),
        pltpu.VMEM((2, steps, RING - 1, strip, HALF), BF16),
        pltpu.VMEM((2, steps, strip, HALF), BF16), pltpu.VMEM((2, steps, RUN - 1, strip, PIECE), BF16),
        pltpu.VMEM((steps, strip, PIECE), F32),
        pltpu.VMEM((steps, tokens, HALF), BF16), pltpu.VMEM((steps, tokens, HALF), BF16),
        dma((4,)),
    ]
    scratch += [dma((steps,)), dma((steps,)), dma((steps,)), dma((steps + 1,)), dma((blocks // 2,))]
    scratch += [dma((2, steps)), dma((2, steps)), dma((steps + 1,)), dma((steps,)), dma((steps,)), dma((steps,))]
    scratch += [dma(())] * 11 + [pltpu.SemaphoreType.REGULAR]
    near = pltpu.VMEM((rows, width), BF16)
    params_next, tracker_next = pl.pallas_call(
        step_kernel,
        out_shape=(near, near),
        in_specs=[any_] * 4,
        out_specs=[pl.BlockSpec(memory_space=pltpu.VMEM)] * 2,
        scratch_shapes=scratch,
        name="tracking_step",
        compiler_params=pltpu.CompilerParams(collective_id=0, has_side_effects=True, vmem_limit_bytes=59 << 20),
    )(params[0], tracker[0], hidden.T, target)
    far = jax.ShapeDtypeStruct((rows, width), BF16)
    params_next, tracker_next = pl.pallas_call(
        store_kernel,
        out_shape=(far, far),
        in_specs=[any_] * 2,
        out_specs=(any_, any_),
        scratch_shapes=[dma((2,))],
        name="store",
        compiler_params=pltpu.CompilerParams(vmem_limit_bytes=1 << 20),
    )(params_next, tracker_next)
    return params_next[None], tracker_next[None]


def solution(mesh):
    placed = (P("grp", "blk", None), P("grp", "blk", None), P("grp", "blk"), P("grp", None))
    return jax.shard_map(
        body,
        mesh=mesh,
        in_specs=placed,
        out_specs=(P("grp", "blk", None), P("grp", "blk", None)),
        check_vma=False,
    )
```
